32 devices in a mesh: row: 4 (over x, core), col: 8 (over z, y).
Axes of the slice: x: 2, y: 2, z: 4, core: 2. Of those that a mesh axis runs over, the one named last changes fastest.
Arguments:
- users: bfloat16 [32768, 256], P(('row', 'col')), may hold values from -20 to 20
- positives: int32 [32768], P(('row', 'col')), may hold values from 0 to 511
- items: bfloat16 [512, 256], P(('row', 'col')), may hold values from -6 to 6
- item_ids: int32 [512], P(('row', 'col')), may hold values from 0 to 999999
Outputs:
- loss: float32 [32768], P(('row', 'col'))
The draws below stay inside these ranges and needn't reach their ends.
All inputs are finite; a program needn't handle non-finite values.
Results may differ from the reference program's by a relative error of at most 0.0003.
Values may be sent and summed in bfloat16 or wider, within the bound.
A program may use at most 128 MiB of HBM per device.

```python
import math
import jax
import jax.numpy as jnp
import numpy as np
from jax import lax

E = 256
ITEMS_DEV = 16
USERS = 32768
ITEMS = 512


def drawn(key):
    item_key = jax.random.fold_in(key, 11)
    user_key = jax.random.fold_in(key, 12)
    items = jnp.clip(jax.random.normal(item_key, (ITEMS, E), jnp.float32), -6.0, 6.0)
    users = jnp.clip(jax.random.normal(user_key, (USERS, E), jnp.float32), -6.0, 6.0)
    return (users, items)


def draw_users(key, part):
    return drawn(key)[0].astype(jnp.bfloat16)


def draw_items(key, part):
    return drawn(key)[1].astype(jnp.bfloat16)


def place_ends(drawn, own_key, low, high):
    spot = [jax.random.randint(jax.random.fold_in(own_key, axis), (), 0, length) for axis, length in enumerate(drawn.shape)]
    widest = drawn.shape.index(max(drawn.shape))
    neighbour = spot[:widest] + [(spot[widest] + 1) % drawn.shape[widest]] + spot[widest + 1:]
    return drawn.at[tuple(spot)].set(low).at[tuple(neighbour)].set(high)


def wide_ids(rng, shape, count, lean):
    portions = [min(1 << octave, count + 1 - (1 << octave)) * (1 << 20) // math.isqrt((1 << octave) ** lean) + 1 for octave in range((count + 1).bit_length()) if 1 << octave <= count]
    scale = 1 + sum(portions) // (1 << 30)
    listing = np.cumsum(np.array([max(1, weight // scale) for weight in portions]))
    ticket = jax.random.randint(jax.random.fold_in(rng, 1), shape, 0, int(listing[len(portions) - 1]))
    start = jnp.left_shift(1, jnp.searchsorted(jnp.asarray(listing, jnp.int32), ticket, side="right").astype(jnp.int32))
    rank = start - 1 + jax.random.randint(jax.random.fold_in(rng, 4), shape, 0, 1 << 30) % jnp.minimum(start, count + 1 - start)
    return jax.random.permutation(jax.random.fold_in(rng, 2), count)[rank].astype(jnp.int32)


def setup_inputs(seed: int = 0) -> dict:
    key_list = jax.random.split(jax.random.key(seed), 5)
    users = draw_users(jax.random.fold_in(key_list[4], 71), 0)
    positives = place_ends(jax.random.randint(key_list[1], (USERS,), 0, ITEMS), jax.random.fold_in(key_list[1], 1), 0, ITEMS - 1).astype(jnp.int32)
    items = draw_items(jax.random.fold_in(key_list[4], 71), 0)
    item_ids = place_ends(wide_ids(key_list[3], (ITEMS,), 1000000, 2), jax.random.fold_in(key_list[3], 3), 0, 999999).astype(jnp.int32)
    return {"users": users, "positives": positives, "items": items, "item_ids": item_ids}


def reference(users, positives, items, item_ids):
    pos_id = item_ids[positives]
    block = ITEMS_DEV * 8
    count = ITEMS // block
    init = (jnp.full((USERS,), -1e30, jnp.float32), jnp.zeros((USERS,), jnp.float32), jnp.zeros((USERS,), jnp.float32))

    def step(carry, index):
        high, summed, chosen = carry
        start = (index * block).astype(jnp.int32)
        piece = lax.dynamic_slice_in_dim(items, start, block, 0)
        ids = lax.dynamic_slice_in_dim(item_ids, start, block, 0)
        where_at = start + jnp.arange(block, dtype=jnp.int32)
        scores = 0.125 * jnp.dot(users, piece.T, preferred_element_type=jnp.float32)
        hit = where_at[None, :] == positives[:, None]
        keep = (ids[None, :] != pos_id[:, None]) | hit
        masked = jnp.where(keep, scores, -1e30)
        new_high = jnp.maximum(high, jnp.max(masked, axis=1))
        terms = jnp.where(keep, jnp.exp(masked - new_high[:, None]), 0.0)
        summed = summed * jnp.exp(high - new_high) + jnp.sum(terms, axis=1)
        chosen = chosen + jnp.sum(jnp.where(hit, scores, 0.0), axis=1)
        return (new_high, summed, chosen), None

    carry, _ = lax.scan(step, init, jnp.arange(count, dtype=jnp.int32))
    high, summed, chosen = carry
    return high + jnp.log(summed) - chosen
```

```python
import functools
import math

import jax
import jax.numpy as jnp
from jax import lax
from jax.experimental import pallas as pl
from jax.experimental.pallas import tpu as pltpu
from jax.sharding import PartitionSpec as P

MESH = pl.DeviceIdType.MESH
TWO_LEVEL = False
LOG2E = math.log2(math.e)
LOW = -1e30


def div(a, b):
    return a // b if isinstance(a, int) else lax.div(a, jnp.int32(b))


def rem(a, b):
    return a % b if isinstance(a, int) else lax.rem(a, jnp.int32(b))


def flip(z, k, n):
    if n & (n - 1):
        return rem(z + k, n)
    out, bit = 0, 1
    while bit < n:
        out = out + bit * rem(rem(div(z, bit), 2) + rem(div(k, bit), 2), 2)
        bit *= 2
    return out


def loop(n, body, limit=64):
    if n <= limit:
        for i in range(n):
            body(i)
    else:
        lax.fori_loop(0, n, lambda i, c: (body(i), c)[1], 0)


def kernel(nrow, ncol, users_hbm, pos_hbm, items_hbm, ids_hbm, out_ref,
           users, pos, pool, ids, tab, state, local_sem, send_sem, recv_sem,
           id_send, id_recv):
    ny = 2 if ncol % 2 == 0 else 1
    nz = ncol // ny
    group = nrow * ny
    count = nrow * ncol
    depth = pool.shape[1]
    chunks = users.shape[0] // 128
    rows = group * depth
    row, col = lax.axis_index("row"), lax.axis_index("col")
    z, y = div(col, ny), rem(col, ny)

    def slot_of(r, zi, yi):
        return zi * group + r * ny + yi

    mine = slot_of(row, z, y)

    def peer(k):
        kz, q = div(k, group), rem(k, group)
        r = rem(row + div(q, ny), nrow)
        yi = rem(y + rem(q, ny), ny)
        zi = flip(z, kz, nz)
        return r, zi * ny + yi, slot_of(r, zi, yi)

    own = pltpu.make_async_copy(items_hbm, pool.at[mine], local_sem.at[0])
    own_ids = pltpu.make_async_copy(ids_hbm, ids.at[mine], local_sem.at[1])
    own_users = pltpu.make_async_copy(users_hbm, users, local_sem.at[2])
    own_pos = pltpu.make_async_copy(pos_hbm, pos, local_sem.at[3])
    own_ids.start()
    own.start()
    own_pos.start()
    own_users.start()

    barrier = pltpu.get_barrier_semaphore()

    def greet(i):
        r, c, _ = peer(i + 1)
        pl.semaphore_signal(barrier, inc=1, device_id=(r, c), device_id_type=MESH)

    loop(count - 1, greet)
    own_ids.wait()
    own.wait()
    pl.semaphore_wait(barrier, count - 1)

    def id_copy(k):
        r, c, s = peer(k)
        return pltpu.make_async_remote_copy(
            src_ref=ids.at[mine], dst_ref=ids.at[mine], send_sem=id_send.at[s],
            recv_sem=id_recv.at[mine], device_id=(r, c), device_id_type=MESH)

    def item_copy(k):
        r, c, s = peer(k)
        return pltpu.make_async_remote_copy(
            src_ref=pool.at[mine], dst_ref=pool.at[mine], send_sem=send_sem.at[s],
            recv_sem=recv_sem.at[mine], device_id=(r, c), device_id_type=MESH)

    def arrival(buf, sems, s):
        return pltpu.make_async_copy(buf.at[s], buf.at[s], sems.at[s])

    loop(count - 1, lambda i: id_copy(count - 1 - i).start())
    loop(count - 1, lambda i: item_copy(count - 1 - i).start())

    own_pos.wait()
    p = pos[...]
    d, lane = p // depth, p % depth
    r, c = d // ncol, d % ncol
    slot = (c // ny) * group + r * ny + c % ny
    place = slot * depth + lane

    state[0] = jnp.full(state.shape[1:], LOW, jnp.float32)
    state[1] = jnp.zeros(state.shape[1:], jnp.float32)
    state[2] = jnp.zeros(state.shape[1:], jnp.float32)

    def wait_ids(i):
        _, _, s = peer(i + 1)
        arrival(ids, id_recv, s).wait()

    loop(count - 1, wait_ids)
    flat = ids[...].reshape(count, depth)
    tab[...] = jnp.concatenate(
        [flat, jnp.zeros((count, 128 - depth), jnp.int32)], axis=1)

    def look(t, found):
        line = jnp.broadcast_to(tab[pl.ds(t, 1), :], p.shape)
        got = jnp.take_along_axis(line, lane, axis=1, mode="promise_in_bounds")
        return jnp.where(slot == t, got, found)

    pid = jnp.zeros(p.shape, jnp.int32)
    if count <= 64:
        for t in range(count):
            pid = look(t, pid)
    else:
        pid = lax.fori_loop(0, count, look, pid)
    pid = pid.astype(jnp.float32)

    own_users.wait()
    eye = (lax.broadcasted_iota(jnp.int32, (1, depth, depth), 1)
           == lax.broadcasted_iota(jnp.int32, (1, depth, depth), 2))

    def absorb(kz):
        zi = flip(z, kz, nz)

        def wait_items(q):
            _, _, s = peer(kz * group + q)
            if isinstance(kz, int) and isinstance(q, int):
                if kz == 0 and q == 0:
                    return
                arrival(pool, recv_sem, s).wait()
            else:
                @pl.when(kz * group + q > 0)
                def _():
                    arrival(pool, recv_sem, s).wait()

        loop(group, wait_items)
        block = pool[pl.ds(zi * group, group)].reshape(rows, pool.shape[2])
        names = ids[pl.ds(zi * group, group)].astype(jnp.float32)
        names = jnp.broadcast_to(names, (group, depth, depth))
        names = jnp.sum(jnp.where(eye, names, 0.0), axis=2, keepdims=True)
        names = jnp.broadcast_to(names.reshape(rows, 1), (rows, 128))
        at = lax.broadcasted_iota(jnp.int32, (rows, 128), 0)
        here = place - zi * rows
        for i in range(chunks):
            x = lax.dot_general(
                block, users[pl.ds(i * 128, 128), :], (((1,), (1,)), ((), ())),
                preferred_element_type=jnp.float32) * (0.125 * LOG2E)
            hit = at == here[i:i + 1, :]
            keep = (names != pid[i:i + 1, :]) | hit
            masked = jnp.where(keep, x, LOW).reshape(rows // 8, 8, 128)
            high = state[0, i]
            top = jnp.maximum(high, jnp.max(masked, axis=0))
            terms = jnp.sum(jnp.exp2(masked - top[None]), axis=0)
            state[1, i] = state[1, i] * jnp.exp2(high - top) + terms
            state[0, i] = top
            state[2, i] = state[2, i] + jnp.sum(
                jnp.where(hit, x, 0.0).reshape(rows // 8, 8, 128), axis=0)

    loop(nz, absorb, 4)

    for i in range(chunks):
        high = state[0, i]
        top = jnp.max(high, axis=0, keepdims=True)
        total = jnp.sum(state[1, i] * jnp.exp2(high - top), axis=0, keepdims=True)
        chosen = jnp.sum(state[2, i], axis=0, keepdims=True)
        out_ref[i:i + 1, :] = (top - chosen) * (1.0 / LOG2E) + jnp.log(total)

    def finish(i):
        id_copy(i + 1).wait_send()
        item_copy(i + 1).wait_send()

    loop(count - 1, finish)


def solution(mesh):
    nrow, ncol = mesh.shape["row"], mesh.shape["col"]
    count = nrow * ncol

    def per_device(users, positives, items, item_ids):
        n, width = users.shape
        depth = items.shape[0]
        lines = n // 128
        out = pl.pallas_call(
            functools.partial(kernel, nrow, ncol),
            out_shape=jax.ShapeDtypeStruct((lines, 128), jnp.float32),
            in_specs=[pl.BlockSpec(memory_space=pl.ANY)] * 4,
            out_specs=pl.BlockSpec(memory_space=pltpu.VMEM),
            scratch_shapes=[
                pltpu.VMEM((n, width), users.dtype),
                pltpu.VMEM((lines, 128), jnp.int32),
                pltpu.VMEM((count, depth, width), items.dtype),
                pltpu.VMEM((count, 1, depth), jnp.int32),
                pltpu.VMEM((count, 128), jnp.int32),
                pltpu.VMEM((3, lines, 8, 128), jnp.float32),
                pltpu.SemaphoreType.DMA((4,)),
                pltpu.SemaphoreType.DMA((count,)),
                pltpu.SemaphoreType.DMA((count,)),
                pltpu.SemaphoreType.DMA((count,)),
                pltpu.SemaphoreType.DMA((count,)),
            ],
            compiler_params=pltpu.CompilerParams(
                collective_id=0, has_side_effects=True),
        )(users, positives.reshape(lines, 128), items, item_ids.reshape(1, depth))
        return out.reshape(n)

    in_specs = (
        P(("row", "col"), None),
        P(("row", "col")),
        P(("row", "col"), None),
        P(("row", "col")),
    )
    return jax.shard_map(
        per_device, mesh=mesh, in_specs=in_specs, out_specs=P(("row", "col")),
        check_vma=False)
```

```python
import functools
import math

import jax
import jax.numpy as jnp
from jax import lax
from jax.experimental import pallas as pl
from jax.experimental.pallas import tpu as pltpu
from jax.sharding import PartitionSpec as P

MESH = pl.DeviceIdType.MESH
LOG2E = math.log2(math.e)
LOW = -1e30


def div(a, b):
    return a // b if isinstance(a, int) else lax.div(a, jnp.int32(b))


def rem(a, b):
    return a % b if isinstance(a, int) else lax.rem(a, jnp.int32(b))


def flip(z, k, n):
    if n & (n - 1):
        return rem(z + k, n)
    out, bit = 0, 1
    while bit < n:
        out = out + bit * rem(rem(div(z, bit), 2) + rem(div(k, bit), 2), 2)
        bit *= 2
    return out


def loop(n, body, limit=64):
    if n <= limit:
        for i in range(n):
            body(i)
    else:
        lax.fori_loop(0, n, lambda i, c: (body(i), c)[1], 0)


def kernel(nrow, ncol, users_hbm, pos_hbm, items_hbm, ids_hbm, out_ref,
           users, pos, pool, ids, tab, state, local_sem, send_sem, recv_sem,
           id_send, id_recv):
    ny = 2 if ncol % 2 == 0 else 1
    nz = ncol // ny
    group = nrow * ny
    count = nrow * ncol
    depth = pool.shape[1]
    chunks = users.shape[0] // 128
    rows = group * depth
    row, col = lax.axis_index("row"), lax.axis_index("col")
    z, y = div(col, ny), rem(col, ny)

    def slot_of(r, zi, yi):
        return zi * group + r * ny + yi

    mine = slot_of(row, z, y)

    core = rem(row, 2)
    fan = nrow // 2 * ny
    chips = nz * fan
    mate = (row + 1 - 2 * core, col)

    def chip(k):
        kz, q = div(k, fan), rem(k, fan)
        r = rem(div(row, 2) + div(q, ny), nrow // 2) * 2 + core
        yi = rem(y + rem(q, ny), ny)
        zi = flip(z, kz, nz)
        return r, zi * ny + yi, slot_of(r, zi, yi)

    def mate_slot(k):
        return chip(k)[2] + (1 - 2 * core) * ny

    own = pltpu.make_async_copy(items_hbm, pool.at[mine], local_sem.at[0])
    own_ids = pltpu.make_async_copy(ids_hbm, ids.at[mine], local_sem.at[1])
    own_users = pltpu.make_async_copy(users_hbm, users, local_sem.at[2])
    own_pos = pltpu.make_async_copy(pos_hbm, pos, local_sem.at[3])
    own_ids.start()
    own.start()
    own_pos.start()
    own_users.start()

    barrier = pltpu.get_barrier_semaphore()

    def greet(i):
        r, c, _ = chip(chips - 1 - i)
        pl.semaphore_signal(barrier, inc=1, device_id=(r, c), device_id_type=MESH)

    loop(chips - 1, greet)
    pl.semaphore_signal(barrier, inc=1, device_id=mate, device_id_type=MESH)
    own_ids.wait()
    own.wait()
    pl.semaphore_wait(barrier, chips)

    def push(buf, sends, recvs, s, n, r, c):
        return pltpu.make_async_remote_copy(
            src_ref=buf.at[s], dst_ref=buf.at[s], send_sem=sends.at[n],
            recv_sem=recvs.at[s], device_id=(r, c), device_id_type=MESH)

    def id_out(k):
        r, c, _ = chip(k)
        return push(ids, id_send, id_recv, mine, k, r, c)

    def item_out(k):
        r, c, _ = chip(k)
        return push(pool, send_sem, recv_sem, mine, k, r, c)

    def id_over(k):
        return push(ids, id_send, id_recv, chip(k)[2], chips + k, *mate)

    def item_over(k):
        return push(pool, send_sem, recv_sem, chip(k)[2], chips + k, *mate)

    def arrival(buf, sems, s):
        return pltpu.make_async_copy(buf.at[s], buf.at[s], sems.at[s])

    loop(chips - 1, lambda i: id_out(chips - 1 - i).start())
    loop(chips - 1, lambda i: item_out(chips - 1 - i).start())
    id_over(0).start()
    item_over(0).start()

    own_pos.wait()
    p = pos[...]
    d, lane = p // depth, p % depth
    r, c = d // ncol, d % ncol
    slot = (c // ny) * group + r * ny + c % ny
    place = slot * depth + lane

    state[0] = jnp.full(state.shape[1:], LOW, jnp.float32)
    state[1] = jnp.zeros(state.shape[1:], jnp.float32)
    state[2] = jnp.zeros(state.shape[1:], jnp.float32)

    def relay_ids(i):
        arrival(ids, id_recv, chip(i + 1)[2]).wait()
        id_over(i + 1).start()

    def relay_items(i):
        arrival(pool, recv_sem, chip(i + 1)[2]).wait()
        item_over(i + 1).start()

    loop(chips - 1, relay_ids)
    early = (nz - 1) * fan - 1
    loop(early, relay_items)
    loop(chips, lambda k: arrival(ids, id_recv, mate_slot(k)).wait())
    flat = ids[...].reshape(count, depth)
    tab[...] = jnp.concatenate(
        [flat, jnp.zeros((count, 128 - depth), jnp.int32)], axis=1)

    def look(t, found):
        line = jnp.broadcast_to(tab[pl.ds(t, 1), :], p.shape)
        got = jnp.take_along_axis(line, lane, axis=1, mode="promise_in_bounds")
        return jnp.where(slot == t, got, found)

    pid = jnp.zeros(p.shape, jnp.int32)
    if count <= 64:
        for t in range(count):
            pid = look(t, pid)
    else:
        pid = lax.fori_loop(0, count, look, pid)
    pid = pid.astype(jnp.float32)

    own_users.wait()
    eye = (lax.broadcasted_iota(jnp.int32, (1, depth, depth), 1)
           == lax.broadcasted_iota(jnp.int32, (1, depth, depth), 2))

    def absorb(kz):
        zi = flip(z, kz, nz)

        loop(fan, lambda q: arrival(
            pool, recv_sem, mate_slot(kz * fan + q)).wait())
        block = pool[pl.ds(zi * group, group)].reshape(rows, pool.shape[2])
        names = ids[pl.ds(zi * group, group)].astype(jnp.float32)
        names = jnp.broadcast_to(names, (group, depth, depth))
        names = jnp.sum(jnp.where(eye, names, 0.0), axis=2, keepdims=True)
        names = jnp.broadcast_to(names.reshape(rows, 1), (rows, 128))
        at = lax.broadcasted_iota(jnp.int32, (rows, 128), 0)
        here = place - zi * rows
        for i in range(chunks):
            x = lax.dot_general(
                block, users[pl.ds(i * 128, 128), :], (((1,), (1,)), ((), ())),
                preferred_element_type=jnp.float32) * (0.125 * LOG2E)
            hit = at == here[i:i + 1, :]
            keep = (names != pid[i:i + 1, :]) | hit
            masked = jnp.where(keep, x, LOW).reshape(rows // 8, 8, 128)
            high = state[0, i]
            top = jnp.maximum(high, jnp.max(masked, axis=0))
            terms = jnp.sum(jnp.exp2(masked - top[None]), axis=0)
            state[1, i] = state[1, i] * jnp.exp2(high - top) + terms
            state[0, i] = top
            state[2, i] = state[2, i] + jnp.sum(
                jnp.where(hit, x, 0.0).reshape(rows // 8, 8, 128), axis=0)

    absorb(0)
    loop(fan, lambda q: relay_items(early + q))
    if nz <= 4:
        for kz in range(1, nz):
            absorb(kz)
    else:
        lax.fori_loop(1, nz, lambda kz, c: (absorb(kz), c)[1], 0)

    for i in range(chunks):
        high = state[0, i]
        top = jnp.max(high, axis=0, keepdims=True)
        total = jnp.sum(state[1, i] * jnp.exp2(high - top), axis=0, keepdims=True)
        chosen = jnp.sum(state[2, i], axis=0, keepdims=True)
        out_ref[i:i + 1, :] = (top - chosen) * (1.0 / LOG2E) + jnp.log(total)

    def finish(i):
        id_out(i + 1).wait_send()
        item_out(i + 1).wait_send()

    def finish_over(k):
        id_over(k).wait_send()
        item_over(k).wait_send()

    loop(chips - 1, finish)
    loop(chips, finish_over)


def solution(mesh):
    nrow, ncol = mesh.shape["row"], mesh.shape["col"]
    count = nrow * ncol

    def per_device(users, positives, items, item_ids):
        n, width = users.shape
        depth = items.shape[0]
        lines = n // 128
        out = pl.pallas_call(
            functools.partial(kernel, nrow, ncol),
            out_shape=pltpu.VMEM((lines, 128), jnp.float32),
            in_specs=[pl.BlockSpec(memory_space=pl.ANY)] * 4,
            out_specs=pl.BlockSpec(memory_space=pltpu.VMEM),
            scratch_shapes=[
                pltpu.VMEM((n, width), users.dtype),
                pltpu.VMEM((lines, 128), jnp.int32),
                pltpu.VMEM((count, depth, width), items.dtype),
                pltpu.VMEM((count, 1, depth), jnp.int32),
                pltpu.VMEM((count, 128), jnp.int32),
                pltpu.VMEM((3, lines, 8, 128), jnp.float32),
                pltpu.SemaphoreType.DMA((4,)),
                pltpu.SemaphoreType.DMA((count,)),
                pltpu.SemaphoreType.DMA((count,)),
                pltpu.SemaphoreType.DMA((count,)),
                pltpu.SemaphoreType.DMA((count,)),
            ],
            compiler_params=pltpu.CompilerParams(
                collective_id=0, has_side_effects=True),
        )(users, positives.reshape(lines, 128), items, item_ids.reshape(1, depth))
        return out.reshape(n)

    in_specs = (
        P(("row", "col"), None),
        P(("row", "col")),
        P(("row", "col"), None),
        P(("row", "col")),
    )
    return jax.shard_map(
        per_device, mesh=mesh, in_specs=in_specs, out_specs=P(("row", "col")),
        check_vma=False)
```
